64 devices in a mesh: dp: 4 (over x, y), tp: 16 (over z, core).
Axes of the slice: x: 2, y: 2, z: 8, core: 2. Of those that a mesh axis runs over, the one named last changes fastest.
The devices are a block of a 4x4x8 slice.
Arguments:
- x: bfloat16 [4, 256, 4096], P('dp', 'tp'), parts along dimension 0
- ln_gain: bfloat16 [2, 4096], replicated
- ln_bias: bfloat16 [2, 4096], replicated
- w_q: bfloat16 [2, 4096, 16, 256], P(None, None, 'tp')
- b_q: bfloat16 [2, 16, 256], P(None, 'tp')
- w_k: bfloat16 [2, 4096, 16, 256], P(None, None, 'tp')
- b_k: bfloat16 [2, 16, 256], P(None, 'tp')
- w_v: bfloat16 [2, 4096, 16, 256], P(None, None, 'tp')
- b_v: bfloat16 [2, 16, 256], P(None, 'tp')
- w_o: bfloat16 [2, 16, 256, 4096], P(None, 'tp')
- b_o: bfloat16 [2, 4096], replicated
- w_up: bfloat16 [2, 4096, 16384], P(None, None, 'tp')
- b_up: bfloat16 [2, 16384], P(None, 'tp')
- w_down: bfloat16 [2, 16384, 4096], P(None, 'tp')
- b_down: bfloat16 [2, 4096], replicated
Outputs:
- output: bfloat16 [4, 256, 4096], P('dp', 'tp'), parts along dimension 0
There are 4 independent parts. The reference program is written for one: setup_inputs(seed, part) draws one part's arguments, and reference() takes and returns one part's arrays. A program takes and returns all parts, laid end to end along the dimension named above; an argument that names none is the same for every part.
All inputs are finite; a program needn't handle non-finite values.
Results may differ from the reference program's by a relative error of at most 0.02.
Values are sent between devices in bfloat16 or wider.
A program may use at most 768 MiB of HBM per device.

```python
import jax
import jax.numpy as jnp
from jax import lax

N_BATCH = 1
SEQ_LEN = 256
D_MODEL = 4096
N_HEADS = 16
HEAD_DIM = 256
D_FF = 16384
ROT_DIM = 32
N_LAYERS = 2


def setup_inputs(seed: int = 0, part: int = 0) -> dict:
    shared_keys = jax.random.split(jax.random.key(seed), 14)
    token_key = jax.random.fold_in(jax.random.key(seed + 1), part)

    def draw(key_index, shape, scale, offset):
        sample = jax.random.normal(shared_keys[key_index], shape, jnp.float32)
        return (offset + scale * sample).astype(jnp.bfloat16)

    proj_shape = (N_LAYERS, D_MODEL, N_HEADS, HEAD_DIM)
    head_shape = (N_LAYERS, N_HEADS, HEAD_DIM)
    wide_shape = (N_LAYERS, D_MODEL)
    in_scale = D_MODEL ** -0.5
    x = jax.random.normal(token_key, (N_BATCH, SEQ_LEN, D_MODEL), jnp.float32).astype(jnp.bfloat16)
    return {
        "x": x,
        "ln_gain": draw(0, wide_shape, 0.3, 1.0),
        "ln_bias": draw(1, wide_shape, 0.3, 0.0),
        "w_q": draw(2, proj_shape, 2.0 * in_scale, 0.0),
        "b_q": draw(3, head_shape, 0.5, 0.0),
        "w_k": draw(4, proj_shape, 2.0 * in_scale, 0.0),
        "b_k": draw(5, head_shape, 0.5, 0.0),
        "w_v": draw(6, proj_shape, in_scale, 0.0),
        "b_v": draw(7, head_shape, 0.5, 0.0),
        "w_o": draw(8, (N_LAYERS, N_HEADS, HEAD_DIM, D_MODEL), in_scale, 0.0),
        "b_o": draw(9, wide_shape, 0.5, 0.0),
        "w_up": draw(10, (N_LAYERS, D_MODEL, D_FF), in_scale, 0.0),
        "b_up": draw(11, (N_LAYERS, D_FF), 0.5, 0.0),
        "w_down": draw(12, (N_LAYERS, D_FF, D_MODEL), D_FF ** -0.5, 0.0),
        "b_down": draw(13, wide_shape, 0.5, 0.0),
    }


def rotary_tables():
    half = ROT_DIM // 2
    inv_freq = 1.0 / (10000.0 ** (jnp.arange(half, dtype=jnp.float32) * (2.0 / ROT_DIM)))
    angles = jnp.arange(SEQ_LEN, dtype=jnp.float32)[:, None] * inv_freq[None, :]
    return jnp.cos(angles)[:, None, :], jnp.sin(angles)[:, None, :]


def apply_rotary(projected, cosine, sine):
    half = ROT_DIM // 2
    first = projected[..., :half]
    second = projected[..., half:ROT_DIM]
    return jnp.concatenate([first * cosine - second * sine, second * cosine + first * sine, projected[..., ROT_DIM:]], axis=-1)


def attend_heads(q_rot, k_rot, values):
    def per_head(operands):
        q_one, k_one, v_one = operands
        scores = jnp.dot(q_one, jnp.transpose(k_one), preferred_element_type=jnp.float32) * (HEAD_DIM ** -0.5)
        causal = jnp.arange(SEQ_LEN)[:, None] >= jnp.arange(SEQ_LEN)[None, :]
        attn_probs = jax.nn.softmax(jnp.where(causal, scores, -1e30), axis=-1).astype(jnp.bfloat16)
        return jnp.dot(attn_probs, v_one, preferred_element_type=jnp.float32).astype(jnp.bfloat16)

    def by_head(tensor):
        return jnp.transpose(tensor, (0, 2, 1, 3)).reshape(N_BATCH * N_HEADS, SEQ_LEN, HEAD_DIM)

    head_out = lax.map(per_head, (by_head(q_rot), by_head(k_rot), by_head(values)))
    return jnp.transpose(head_out.reshape(N_BATCH, N_HEADS, SEQ_LEN, HEAD_DIM), (0, 2, 1, 3))


def layer_forward(hidden, layer_params):
    (ln_gain, ln_bias, w_q, b_q, w_k, b_k, w_v, b_v, w_o, b_o, w_up, b_up, w_down, b_down) = layer_params
    x_f32 = hidden.astype(jnp.float32)
    mean = jnp.mean(x_f32, axis=-1, keepdims=True)
    centered = x_f32 - mean
    variance = jnp.mean(centered * centered, axis=-1, keepdims=True)
    normed = (centered * lax.rsqrt(variance + 1e-5) * ln_gain.astype(jnp.float32) + ln_bias.astype(jnp.float32)).astype(jnp.bfloat16)
    flat = normed.reshape(N_BATCH * SEQ_LEN, D_MODEL)
    head_shape = (N_BATCH, SEQ_LEN, N_HEADS, HEAD_DIM)
    cosine, sine = rotary_tables()

    def project(weight, bias):
        prod = jnp.dot(flat, weight.reshape(D_MODEL, N_HEADS * HEAD_DIM), preferred_element_type=jnp.float32)
        return prod.reshape(head_shape) + bias.astype(jnp.float32)

    q_rot = apply_rotary(project(w_q, b_q), cosine, sine).astype(jnp.bfloat16)
    k_rot = apply_rotary(project(w_k, b_k), cosine, sine).astype(jnp.bfloat16)
    values = project(w_v, b_v).astype(jnp.bfloat16)
    attended = attend_heads(q_rot, k_rot, values)
    dense_out = jnp.dot(attended.reshape(N_BATCH * SEQ_LEN, D_MODEL), w_o.reshape(D_MODEL, D_MODEL), preferred_element_type=jnp.float32)
    up_act = jax.nn.gelu(jnp.dot(flat, w_up, preferred_element_type=jnp.float32) + b_up.astype(jnp.float32), approximate=True).astype(jnp.bfloat16)
    down_out = jnp.dot(up_act, w_down, preferred_element_type=jnp.float32)
    total = x_f32.reshape(N_BATCH * SEQ_LEN, D_MODEL) + dense_out + down_out + b_o.astype(jnp.float32) + b_down.astype(jnp.float32)
    return total.reshape(N_BATCH, SEQ_LEN, D_MODEL).astype(jnp.bfloat16)


def reference(x, ln_gain, ln_bias, w_q, b_q, w_k, b_k, w_v, b_v, w_o, b_o, w_up, b_up, w_down, b_down):
    stacked = (ln_gain, ln_bias, w_q, b_q, w_k, b_k, w_v, b_v, w_o, b_o, w_up, b_up, w_down, b_down)

    def layer_body(hidden, layer_params):
        return layer_forward(hidden, layer_params), None

    final = lax.scan(layer_body, x, stacked)
    return final[0]
```

```python
import functools

import jax
import jax.numpy as jnp
import numpy as np
from jax import lax
from jax.experimental import pallas as pl
from jax.experimental.pallas import tpu as pltpu
from jax.sharding import PartitionSpec as P

ROT_DIM = 32
ROPE_BASE = 10000.0
LN_EPS = 1e-5
MESH = pl.DeviceIdType.MESH
F32 = jnp.float32
BF16 = jnp.bfloat16
CW, CCW = 0, 1


def row_positions(n_chips, rows):
    half, core, chip, row = np.meshgrid(np.arange(2), np.arange(2), np.arange(n_chips), np.arange(rows), indexing="ij")
    return (2 * rows * (2 * chip + core) + rows * half + row).reshape(-1)


def rotary_constants(positions):
    half = ROT_DIM // 2
    inv_freq = (1.0 / (np.float32(ROPE_BASE) ** (np.arange(half, dtype=np.float32) * np.float32(2.0 / ROT_DIM)))).astype(np.float32)
    angles = positions.astype(np.float32)[:, None] * inv_freq[None, :]
    cosine, sine = np.cos(angles), np.sin(angles)
    table = np.zeros((3, positions.size, 128), np.float32)
    table[0] = 1.0
    table[0, :, :half] = cosine
    table[0, :, half:ROT_DIM] = cosine
    table[1, :, :half] = -sine
    table[2, :, half:ROT_DIM] = sine
    return table


def kernel(cfg, x_hbm, gain_ref, lbias_ref, wq, wk, wv, wo, wup, wdown, bq_ref, bk_ref, bv_ref, bup_ref, bo_ref, bdown_ref,
           rot_hbm, mask_hbm, out_hbm,
           xv, gat, par, dbuf, slot, win, wout, qkv, act, rot, mask, outv,
           w_sem, io_sem, ag_s, ag_r, agd_s, agd_r, rsd_s, rsd_r, rs_s, rs_r):
    n_layers, n_chips, rows, width, head, ff = cfg
    half_w = width // 2
    m_rows = 2 * n_chips * rows
    me = lax.axis_index("tp")
    core = lax.rem(me, 2)
    chip = me // 2
    partner = chip * 2 + (1 - core)
    last = n_chips // 2

    def at_chip(offset):
        return lax.rem(chip + offset + 2 * n_chips, n_chips)

    next_dev = (at_chip(1) * 2 + core, at_chip(-1) * 2 + core)

    def cols(ch):
        return pl.ds(ch * half_w, half_w)

    x_copy = pltpu.make_async_copy(x_hbm.at[0], xv, io_sem.at[0])
    x_copy.start()
    rot_copy = pltpu.make_async_copy(rot_hbm, rot, io_sem.at[1])
    mask_copy = pltpu.make_async_copy(mask_hbm, mask, io_sem.at[2])

    def weight_copies(layer):
        copies = []
        for i, src in enumerate((wq, wk, wv)):
            copies.append(pltpu.make_async_copy(src.at[layer], win.at[layer, :, pl.ds(i * head, head)], w_sem.at[layer, i]))
        copies.append(pltpu.make_async_copy(wup.at[layer], win.at[layer, :, pl.ds(3 * head, ff)], w_sem.at[layer, 3]))
        copies.append(pltpu.make_async_copy(wo.at[layer], wout.at[layer, pl.ds(0, head), :], w_sem.at[layer, 4]))
        copies.append(pltpu.make_async_copy(wdown.at[layer], wout.at[layer, pl.ds(head, ff), :], w_sem.at[layer, 5]))
        return copies

    weights = [weight_copies(layer) for layer in range(n_layers)]
    barrier = pltpu.get_barrier_semaphore()
    for dev in (next_dev[CW], next_dev[CCW], partner):
        pl.semaphore_signal(barrier, inc=1, device_id={"tp": dev}, device_id_type=MESH)
    rot_copy.start()
    mask_copy.start()
    for layer in range(n_layers):
        for copy in weights[layer]:
            copy.start()

    def ag_copy(layer, x, d, s, ch):
        src = at_chip(-s if d == CW else s)
        ref = gat.at[layer, x, core, src, :, cols(ch)]
        return pltpu.make_async_remote_copy(ref, ref, ag_s.at[layer, x, d, s, ch], ag_r.at[layer, x, d, s, ch],
                                            device_id={"tp": next_dev[d]}, device_id_type=MESH)

    def agd_copy(layer, x, i, offset):
        ref = gat.at[layer, x, core, at_chip(offset)]
        return pltpu.make_async_remote_copy(ref, ref, agd_s.at[layer, x, i], agd_r.at[layer, x, i],
                                            device_id={"tp": partner}, device_id_type=MESH)

    def ag_incoming(layer, x, d, s, ch):
        src = at_chip(-(s + 1) if d == CW else s + 1)
        ref = gat.at[layer, x, core, src, :, cols(ch)]
        return pltpu.make_async_remote_copy(ref, ref, ag_s.at[layer, x, d, s, ch], ag_r.at[layer, x, d, s, ch],
                                            device_id={"tp": next_dev[d]}, device_id_type=MESH)

    agd_offsets = [0] + [o for s in range(1, last) for o in (-s, s)] + [last]
    pending = []

    def go(copy):
        copy.start()
        pending.append(copy)

    def has_hop(d, s, ch):
        return s < last - 1 or ch == d

    def layer_norm(layer, x):
        value = xv[pl.ds(x * rows, rows), :].astype(F32)
        mean = jnp.mean(value, axis=-1, keepdims=True)
        centered = value - mean
        variance = jnp.mean(centered * centered, axis=-1, keepdims=True)
        normed = centered * lax.rsqrt(variance + LN_EPS) * gain_ref[pl.ds(layer, 1), :].astype(F32) + lbias_ref[pl.ds(layer, 1), :].astype(F32)
        gat[layer, x, core, chip] = normed.astype(BF16)

    def ag_start(layer, x):
        for ch in range(2):
            for d in (CW, CCW):
                go(ag_copy(layer, x, d, 0, ch))
        go(agd_copy(layer, x, 0, 0))

    def ag_hop(layer, x, s):
        for ch in range(2):
            for d in (CW, CCW):
                ag_incoming(layer, x, d, s - 1, ch).wait_recv()
                if has_hop(d, s, ch):
                    go(ag_copy(layer, x, d, s, ch))
        for j, o in enumerate((-s, s)):
            go(agd_copy(layer, x, 2 * s - 1 + j, o))

    def ag_last(layer, x):
        for d in (CW, CCW):
            ag_incoming(layer, x, d, last - 1, d).wait_recv()
        go(agd_copy(layer, x, len(agd_offsets) - 1, last))

    def ag_dwait(layer, x):
        for i, o in enumerate(agd_offsets):
            ref = gat.at[layer, x, 1 - core, at_chip(o)]
            pltpu.make_async_remote_copy(ref, ref, agd_s.at[layer, x, i], agd_r.at[layer, x, i],
                                         device_id={"tp": partner}, device_id_type=MESH).wait_recv()

    def normed_rows(layer, x):
        return gat[layer, x].reshape(m_rows, width)

    def project_qkv(layer, x):
        rows_x = pl.ds(x * m_rows, m_rows)
        out = jnp.dot(normed_rows(layer, x), win[layer, :, pl.ds(0, 3 * head)], preferred_element_type=F32)
        for i, bias in enumerate((bq_ref, bk_ref, bv_ref)):
            value = out[:, i * head:(i + 1) * head] + bias[pl.ds(layer, 1), :].astype(F32)
            if i < 2:
                low = value[:, :128]
                low = (low * rot[0, rows_x, :] + pltpu.roll(low, 128 - ROT_DIM // 2, 1) * rot[1, rows_x, :]
                       + pltpu.roll(low, ROT_DIM // 2, 1) * rot[2, rows_x, :])
                qkv[i, rows_x, pl.ds(0, 128)] = low.astype(BF16)
                qkv[i, rows_x, pl.ds(128, head - 128)] = value[:, 128:].astype(BF16)
            else:
                qkv[i, rows_x, :] = value.astype(BF16)

    def project_up(layer, x, tile, width_n):
        col = pl.ds(tile * width_n, width_n)
        out = jnp.dot(normed_rows(layer, x), win[layer, :, pl.ds(3 * head + tile * width_n, width_n)], preferred_element_type=F32)
        out = out + bup_ref[pl.ds(layer, 1), col].astype(F32)
        act[x, :, pl.ds(head + tile * width_n, width_n)] = jax.nn.gelu(out, approximate=True).astype(BF16)

    def attend():
        scores = lax.dot_general(qkv[0], qkv[1], (((1,), (1,)), ((), ())), preferred_element_type=F32) * (head ** -0.5)
        scores = jnp.where(mask[...] > 0, scores, -1e30)
        top = jnp.max(scores, axis=-1, keepdims=True)
        e = jnp.exp(scores - top)
        probs = (e / jnp.sum(e, axis=-1, keepdims=True)).astype(BF16)
        out = jnp.dot(probs, qkv[2], preferred_element_type=F32).astype(BF16)
        for x in range(2):
            act[x, :, pl.ds(0, head)] = out[x * m_rows:(x + 1) * m_rows]

    def rsd_copy(layer, x, ch):
        return pltpu.make_async_remote_copy(par.at[x, 1 - core, :, :, cols(ch)], dbuf.at[layer, x, :, :, cols(ch)],
                                            rsd_s.at[layer, x, ch], rsd_r.at[layer, x, ch],
                                            device_id={"tp": partner}, device_id_type=MESH)

    def rs_part(layer, x, ch):
        tile = 512 if half_w % 512 == 0 else half_w

        def body(i, carry):
            start = pl.multiple_of(ch * half_w + i * tile, tile)
            out = jnp.dot(act[x], wout[layer, :, pl.ds(start, tile)], preferred_element_type=F32)
            par[x, :, :, :, pl.ds(start, tile)] = out.astype(BF16).reshape(2, n_chips, rows, tile)
            return carry

        lax.fori_loop(0, half_w // tile, body, 0)
        go(rsd_copy(layer, x, ch))

    def rs_copy(layer, x, d, t, ch):
        dest = at_chip(last - t if d == CW else t - last)
        return pltpu.make_async_remote_copy(par.at[x, core, dest, :, cols(ch)], slot.at[layer, x, d, t, :, cols(ch)],
                                            rs_s.at[layer, x, d, t, ch], rs_r.at[layer, x, d, t, ch],
                                            device_id={"tp": next_dev[d]}, device_id_type=MESH)

    def rs_first(d, ch):
        return 0 if ch == d else 1

    def rs_hop(layer, x, d, t, ch):
        dest = at_chip(last - t if d == CW else t - last)
        total = par[x, core, dest, :, cols(ch)].astype(F32) + dbuf[layer, x, dest, :, cols(ch)].astype(F32)
        if t > rs_first(d, ch):
            rs_copy(layer, x, d, t - 1, ch).wait_recv()
            total = total + slot[layer, x, d, t - 1, :, cols(ch)].astype(F32)
        par[x, core, dest, :, cols(ch)] = total.astype(BF16)
        go(rs_copy(layer, x, d, t, ch))

    def rs_begin(layer, x, ch):
        rsd_copy(layer, x, ch).wait_recv()
        for d in (CW, CCW):
            rs_hop(layer, x, d, rs_first(d, ch), ch)

    def rs_step(layer, x, t):
        for ch in range(2):
            for d in (CW, CCW):
                if t > rs_first(d, ch):
                    rs_hop(layer, x, d, t, ch)

    def rs_final(layer, x):
        for ch in range(2):
            total = par[x, core, chip, :, cols(ch)].astype(F32) + dbuf[layer, x, chip, :, cols(ch)].astype(F32)
            for d in (CW, CCW):
                rs_copy(layer, x, d, last - 1, ch).wait_recv()
                total = total + slot[layer, x, d, last - 1, :, cols(ch)].astype(F32)
            total = (total + bo_ref[pl.ds(layer, 1), cols(ch)].astype(F32) + bdown_ref[pl.ds(layer, 1), cols(ch)].astype(F32)
                     + xv[pl.ds(x * rows, rows), cols(ch)].astype(F32))
            target = xv if layer < n_layers - 1 else outv
            target[pl.ds(x * rows, rows), cols(ch)] = total.astype(BF16)

    def drain():
        for copy in pending:
            copy.wait_send()
        pending.clear()

    x_copy.wait()
    for x in range(2):
        layer_norm(0, x)
    pl.semaphore_wait(barrier, 3)
    for x in range(2):
        ag_start(0, x)
    rot_copy.wait()
    mask_copy.wait()
    up_tile = 512 if ff % 512 == 0 else ff
    n_up = ff // up_tile
    for layer in range(n_layers):
        for s in range(1, last):
            for x in range(2):
                ag_hop(layer, x, s)
        ag_last(layer, 0)
        for i in range(3):
            weights[layer][i].wait()
        ag_dwait(layer, 0)
        project_qkv(layer, 0)
        ag_last(layer, 1)
        weights[layer][3].wait()
        for tile in range(n_up):
            project_up(layer, 0, tile, up_tile)
        ag_dwait(layer, 1)
        project_qkv(layer, 1)
        attend()
        for i in (4, 5):
            weights[layer][i].wait()
        rs_part(layer, 0, 0)
        rs_part(layer, 0, 1)
        rs_begin(layer, 0, 0)
        project_up(layer, 1, 0, up_tile)
        rs_begin(layer, 0, 1)
        for tile in range(1, n_up):
            project_up(layer, 1, tile, up_tile)
        rs_step(layer, 0, 1)
        rs_part(layer, 1, 0)
        rs_part(layer, 1, 1)
        rs_step(layer, 0, 2)
        rs_begin(layer, 1, 0)
        rs_begin(layer, 1, 1)
        rs_step(layer, 0, 3)
        for t in range(1, last):
            rs_step(layer, 1, t)
        for x in range(2):
            rs_final(layer, x)
            if layer < n_layers - 1:
                layer_norm(layer + 1, x)
        drain()
        if layer < n_layers - 1:
            for x in range(2):
                ag_start(layer + 1, x)
    out_copy = pltpu.make_async_copy(outv, out_hbm.at[0], io_sem.at[3])
    out_copy.start()
    out_copy.wait()


def solution(mesh):
    tp = mesh.shape["tp"]
    n_chips = tp // 2
    head_spec = P(None, None, "tp", None)
    head_bias_spec = P(None, "tp", None)
    in_specs = (P("dp", "tp", None), P(), P(), head_spec, head_bias_spec, head_spec, head_bias_spec, head_spec, head_bias_spec,
                P(None, "tp", None, None), P(), P(None, None, "tp"), P(None, "tp"), P(None, "tp", None), P())

    def local_program(x_loc, ln_gain, ln_bias, w_q, b_q, w_k, b_k, w_v, b_v, w_o, b_o, w_up, b_up, w_down, b_down):
        n_layers, width, _, head = w_q.shape
        ff = w_up.shape[2]
        rows = x_loc.shape[1] // 2
        m_rows = 2 * n_chips * rows
        positions = row_positions(n_chips, rows)
        rot = jnp.asarray(rotary_constants(positions))
        mask = jnp.asarray((positions[:, None] >= positions[None, :]).astype(np.float32))
        flat = lambda w: w.reshape(n_layers, width, head)
        bias = lambda b: b.reshape(n_layers, head)
        cfg = (n_layers, n_chips, rows, width, head, ff)
        any_spec = pl.BlockSpec(memory_space=pl.ANY)
        vmem_spec = pl.BlockSpec(memory_space=pltpu.VMEM)
        dma = pltpu.SemaphoreType.DMA
        hops = n_chips // 2
        return pl.pallas_call(
            functools.partial(kernel, cfg),
            out_shape=jax.ShapeDtypeStruct(x_loc.shape, x_loc.dtype),
            in_specs=[any_spec, vmem_spec, vmem_spec] + [any_spec] * 6 + [vmem_spec] * 6 + [any_spec] * 2,
            out_specs=any_spec,
            scratch_shapes=[
                pltpu.VMEM((2 * rows, width), BF16),
                pltpu.VMEM((n_layers, 2, 2, n_chips, rows, width), BF16),
                pltpu.VMEM((2, 2, n_chips, rows, width), BF16),
                pltpu.VMEM((n_layers, 2, n_chips, rows, width), BF16),
                pltpu.VMEM((n_layers, 2, 2, hops, rows, width), BF16),
                pltpu.VMEM((n_layers, width, 3 * head + ff), BF16),
                pltpu.VMEM((n_layers, head + ff, width), BF16),
                pltpu.VMEM((3, 2 * m_rows, head), BF16),
                pltpu.VMEM((2, m_rows, head + ff), BF16),
                pltpu.VMEM((3, 2 * m_rows, 128), F32),
                pltpu.VMEM((2 * m_rows, 2 * m_rows), F32),
                pltpu.VMEM((2 * rows, width), BF16),
                dma((n_layers, 6)),
                dma((4,)),
                dma((n_layers, 2, 2, hops, 2)),
                dma((n_layers, 2, 2, hops, 2)),
                dma((n_layers, 2, n_chips)),
                dma((n_layers, 2, n_chips)),
                dma((n_layers, 2, 2)),
                dma((n_layers, 2, 2)),
                dma((n_layers, 2, 2, hops, 2)),
                dma((n_layers, 2, 2, hops, 2)),
            ],
            compiler_params=pltpu.CompilerParams(collective_id=0, has_side_effects=True, vmem_limit_bytes=67_000_000),
            name="decoder",
        )(x_loc, ln_gain, ln_bias, flat(w_q), flat(w_k), flat(w_v), w_o.reshape(n_layers, head, width), w_up, w_down,
          bias(b_q), bias(b_k), bias(b_v), b_up, b_o, b_down, rot, mask)

    return jax.shard_map(local_program, mesh=mesh, in_specs=in_specs, out_specs=P("dp", "tp", None), check_vma=False)
```

```python
import functools

import jax
import jax.numpy as jnp
import numpy as np
from jax import lax
from jax.experimental import pallas as pl
from jax.experimental.pallas import tpu as pltpu
from jax.sharding import PartitionSpec as P

ROT_DIM = 32
ROPE_BASE = 10000.0
LN_EPS = 1e-5
MESH = pl.DeviceIdType.MESH
F32 = jnp.float32
BF16 = jnp.bfloat16
CW, CCW = 0, 1
CHUNKS = 4


def row_positions(n_chips, rows):
    half, core, chip, row = np.meshgrid(np.arange(2), np.arange(2), np.arange(n_chips), np.arange(rows), indexing="ij")
    return (2 * rows * (2 * chip + core) + rows * half + row).reshape(-1)


def rotary_constants(positions):
    half = ROT_DIM // 2
    inv_freq = (1.0 / (np.float32(ROPE_BASE) ** (np.arange(half, dtype=np.float32) * np.float32(2.0 / ROT_DIM)))).astype(np.float32)
    angles = positions.astype(np.float32)[:, None] * inv_freq[None, :]
    cosine, sine = np.cos(angles), np.sin(angles)
    table = np.zeros((3, positions.size, 128), np.float32)
    table[0] = 1.0
    table[0, :, :half] = cosine
    table[0, :, half:ROT_DIM] = cosine
    table[1, :, :half] = -sine
    table[2, :, half:ROT_DIM] = sine
    return table


def kernel(cfg, x_hbm, gain_ref, lbias_ref, wq, wk, wv, wo, wup, wdown, bq_ref, bk_ref, bv_ref, bup_ref, bo_ref, bdown_ref,
           rot_hbm, mask_hbm, out_hbm,
           xv, gat, par, dbuf, slot, win, wout, qkv, act, rot, mask, outv,
           w_sem, io_sem, ag_s, ag_r, agd_s, agd_r, rsd_s, rsd_r, rs_s, rs_r):
    n_layers, n_chips, rows, width, head, ff = cfg
    half_w = width // 2
    m_rows = 2 * n_chips * rows
    me = lax.axis_index("tp")
    core = lax.rem(me, 2)
    chip = me // 2
    partner = chip * 2 + (1 - core)
    last = n_chips // 2

    def at_chip(offset):
        return lax.rem(chip + offset + 2 * n_chips, n_chips)

    next_dev = (at_chip(1) * 2 + core, at_chip(-1) * 2 + core)

    def cols(ch):
        return pl.ds(ch * half_w, half_w)

    chunk_w = width // CHUNKS

    def chunk(q):
        return pl.ds(q * chunk_w, chunk_w)

    def owner(q):
        return q * 2 // CHUNKS

    x_copy = pltpu.make_async_copy(x_hbm.at[0], xv, io_sem.at[0])
    x_copy.start()
    rot_copy = pltpu.make_async_copy(rot_hbm, rot, io_sem.at[1])
    mask_copy = pltpu.make_async_copy(mask_hbm, mask, io_sem.at[2])

    def weight_copies(layer):
        copies = []
        for i, src in enumerate((wq, wk, wv)):
            copies.append(pltpu.make_async_copy(src.at[layer], win.at[layer, :, pl.ds(i * head, head)], w_sem.at[layer, i]))
        copies.append(pltpu.make_async_copy(wup.at[layer], win.at[layer, :, pl.ds(3 * head, ff)], w_sem.at[layer, 3]))
        copies.append(pltpu.make_async_copy(wo.at[layer], wout.at[layer, pl.ds(0, head), :], w_sem.at[layer, 4]))
        copies.append(pltpu.make_async_copy(wdown.at[layer], wout.at[layer, pl.ds(head, ff), :], w_sem.at[layer, 5]))
        return copies

    weights = [weight_copies(layer) for layer in range(n_layers)]
    barrier = pltpu.get_barrier_semaphore()
    for dev in (next_dev[CW], next_dev[CCW], partner):
        pl.semaphore_signal(barrier, inc=1, device_id={"tp": dev}, device_id_type=MESH)
    rot_copy.start()
    mask_copy.start()
    for copy in weights[0]:
        copy.start()

    def ag_copy(layer, x, d, s, ch):
        src = at_chip(-s if d == CW else s)
        ref = gat.at[layer, x, core, src, :, cols(ch)]
        return pltpu.make_async_remote_copy(ref, ref, ag_s.at[layer, x, d, s, ch], ag_r.at[layer, x, d, s, ch],
                                            device_id={"tp": next_dev[d]}, device_id_type=MESH)

    def agd_copy(layer, x, i, offset):
        ref = gat.at[layer, x, core, at_chip(offset)]
        return pltpu.make_async_remote_copy(ref, ref, agd_s.at[layer, x, i], agd_r.at[layer, x, i],
                                            device_id={"tp": partner}, device_id_type=MESH)

    def ag_incoming(layer, x, d, s, ch):
        src = at_chip(-(s + 1) if d == CW else s + 1)
        ref = gat.at[layer, x, core, src, :, cols(ch)]
        return pltpu.make_async_remote_copy(ref, ref, ag_s.at[layer, x, d, s, ch], ag_r.at[layer, x, d, s, ch],
                                            device_id={"tp": next_dev[d]}, device_id_type=MESH)

    agd_offsets = [0] + [o for s in range(1, last) for o in (-s, s)] + [last]
    gather_sends, scatter_sends = [], []

    def go(copy, sends):
        copy.start()
        sends.append(copy)

    def has_hop(d, s, ch):
        return s < last - 1 or ch == d

    def layer_norm(layer, x):
        value = xv[pl.ds(x * rows, rows), :].astype(F32)
        mean = jnp.mean(value, axis=-1, keepdims=True)
        centered = value - mean
        variance = jnp.mean(centered * centered, axis=-1, keepdims=True)
        normed = centered * lax.rsqrt(variance + LN_EPS) * gain_ref[pl.ds(layer, 1), :].astype(F32) + lbias_ref[pl.ds(layer, 1), :].astype(F32)
        gat[layer, x, core, chip] = normed.astype(BF16)

    def ag_start(layer, x):
        for ch in range(2):
            for d in (CW, CCW):
                go(ag_copy(layer, x, d, 0, ch), gather_sends)
        go(agd_copy(layer, x, 0, 0), gather_sends)

    def ag_hop(layer, x, s):
        for ch in range(2):
            for d in (CW, CCW):
                ag_incoming(layer, x, d, s - 1, ch).wait_recv()
                if has_hop(d, s, ch):
                    go(ag_copy(layer, x, d, s, ch), gather_sends)
        for j, o in enumerate((-s, s)):
            go(agd_copy(layer, x, 2 * s - 1 + j, o), gather_sends)

    def ag_last(layer, x):
        for d in (CW, CCW):
            ag_incoming(layer, x, d, last - 1, d).wait_recv()
        go(agd_copy(layer, x, len(agd_offsets) - 1, last), gather_sends)

    def ag_dwait(layer, x):
        for i, o in enumerate(agd_offsets):
            ref = gat.at[layer, x, 1 - core, at_chip(o)]
            pltpu.make_async_remote_copy(ref, ref, agd_s.at[layer, x, i], agd_r.at[layer, x, i],
                                         device_id={"tp": partner}, device_id_type=MESH).wait_recv()

    def normed_rows(layer, x):
        return gat[layer, x].reshape(m_rows, width)

    def project_qkv(layer, x):
        rows_x = pl.ds(x * m_rows, m_rows)
        out = jnp.dot(normed_rows(layer, x), win[layer, :, pl.ds(0, 3 * head)], preferred_element_type=F32)
        for i, bias in enumerate((bq_ref, bk_ref, bv_ref)):
            value = out[:, i * head:(i + 1) * head] + bias[pl.ds(layer, 1), :].astype(F32)
            if i < 2:
                low = value[:, :128]
                low = (low * rot[0, rows_x, :] + pltpu.roll(low, 128 - ROT_DIM // 2, 1) * rot[1, rows_x, :]
                       + pltpu.roll(low, ROT_DIM // 2, 1) * rot[2, rows_x, :])
                qkv[i, rows_x, pl.ds(0, 128)] = low.astype(BF16)
                qkv[i, rows_x, pl.ds(128, head - 128)] = value[:, 128:].astype(BF16)
            else:
                qkv[i, rows_x, :] = value.astype(BF16)

    def project_up(layer, x, tile, width_n):
        col = pl.ds(tile * width_n, width_n)
        out = jnp.dot(normed_rows(layer, x), win[layer, :, pl.ds(3 * head + tile * width_n, width_n)], preferred_element_type=F32)
        out = out + bup_ref[pl.ds(layer, 1), col].astype(F32)
        act[x, :, pl.ds(head + tile * width_n, width_n)] = jax.nn.gelu(out, approximate=True).astype(BF16)

    def attend():
        scores = lax.dot_general(qkv[0], qkv[1], (((1,), (1,)), ((), ())), preferred_element_type=F32) * (head ** -0.5)
        scores = jnp.where(mask[...] > 0, scores, -1e30)
        top = jnp.max(scores, axis=-1, keepdims=True)
        e = jnp.exp(scores - top)
        probs = (e / jnp.sum(e, axis=-1, keepdims=True)).astype(BF16)
        out = jnp.dot(probs, qkv[2], preferred_element_type=F32).astype(BF16)
        for x in range(2):
            act[x, :, pl.ds(0, head)] = out[x * m_rows:(x + 1) * m_rows]

    def rsd_copy(layer, x, q):
        return pltpu.make_async_remote_copy(par.at[x, 1 - core, :, :, chunk(q)], dbuf.at[layer, x, :, :, chunk(q)],
                                            rsd_s.at[layer, x, q], rsd_r.at[layer, x, q],
                                            device_id={"tp": partner}, device_id_type=MESH)

    def rs_part(layer, x, q):
        out = jnp.dot(act[x], wout[layer, :, chunk(q)], preferred_element_type=F32)
        par[x, :, :, :, chunk(q)] = out.astype(BF16).reshape(2, n_chips, rows, chunk_w)
        go(rsd_copy(layer, x, q), scatter_sends)

    def rs_copy(layer, x, d, t, q):
        dest = at_chip(last - t if d == CW else t - last)
        return pltpu.make_async_remote_copy(par.at[x, core, dest, :, chunk(q)], slot.at[layer, x, d, t, :, chunk(q)],
                                            rs_s.at[layer, x, d, t, q], rs_r.at[layer, x, d, t, q],
                                            device_id={"tp": next_dev[d]}, device_id_type=MESH)

    def rs_first(d, q):
        return 0 if owner(q) == d else 1

    def rs_hop(layer, x, d, t, q):
        dest = at_chip(last - t if d == CW else t - last)
        total = par[x, core, dest, :, chunk(q)].astype(F32) + dbuf[layer, x, dest, :, chunk(q)].astype(F32)
        if t > rs_first(d, q):
            rs_copy(layer, x, d, t - 1, q).wait_recv()
            total = total + slot[layer, x, d, t - 1, :, chunk(q)].astype(F32)
        par[x, core, dest, :, chunk(q)] = total.astype(BF16)
        go(rs_copy(layer, x, d, t, q), scatter_sends)

    def rs_begin(layer, x, q):
        rsd_copy(layer, x, q).wait_recv()
        for d in (CW, CCW):
            rs_hop(layer, x, d, rs_first(d, q), q)

    def rs_step(layer, x, t, q):
        for d in (CW, CCW):
            if t > rs_first(d, q):
                rs_hop(layer, x, d, t, q)

    def rs_final(layer, x):
        for q in range(CHUNKS):
            total = par[x, core, chip, :, chunk(q)].astype(F32) + dbuf[layer, x, chip, :, chunk(q)].astype(F32)
            for d in (CW, CCW):
                rs_copy(layer, x, d, last - 1, q).wait_recv()
                total = total + slot[layer, x, d, last - 1, :, chunk(q)].astype(F32)
            total = (total + bo_ref[pl.ds(layer, 1), chunk(q)].astype(F32) + bdown_ref[pl.ds(layer, 1), chunk(q)].astype(F32)
                     + xv[pl.ds(x * rows, rows), chunk(q)].astype(F32))
            target = xv if layer < n_layers - 1 else outv
            target[pl.ds(x * rows, rows), chunk(q)] = total.astype(BF16)

    def drain(sends):
        for copy in sends:
            copy.wait_send()
        sends.clear()

    def store(x):
        rows_x = pl.ds(x * rows, rows)
        return pltpu.make_async_copy(outv.at[rows_x], out_hbm.at[0, rows_x], io_sem.at[3 + x])

    def weight_wait(layer, i):
        weights[layer][i].wait()

    def run(event, *place):
        event(*place)

    x_copy.wait()
    for x in range(2):
        run(layer_norm, 0, x)
    pl.semaphore_wait(barrier, 3)
    for x in range(2):
        run(ag_start, 0, x)
    for layer in range(n_layers):
        final = layer == n_layers - 1

        def upper(x, tile, tiles):
            run(project_up, layer, x, tile, ff // tiles)

        def each(event, x, *place):
            for q in place[-1]:
                run(event, layer, x, *place[:-1], q)

        if layer == 0:
            for s in range(1, last):
                for x in range(2):
                    run(ag_hop, layer, x, s)
        else:
            for s in range(2, last):
                for x in range(2):
                    run(ag_hop, layer, x, s)
        run(ag_last, layer, 0)
        if layer == 0:
            rot_copy.wait()
            mask_copy.wait()
            for i in range(3):
                run(weight_wait, layer, i)
        run(ag_dwait, layer, 0)
        run(project_qkv, layer, 0)
        run(ag_last, layer, 1)
        if layer == 0:
            run(weight_wait, layer, 3)
        upper(0, 0, 1)
        run(ag_dwait, layer, 1)
        run(project_qkv, layer, 1)
        run(attend)
        if not final:
            for copy in weights[layer + 1]:
                copy.start()
        run(weight_wait, layer, 4)
        run(weight_wait, layer, 5)
        run(drain, scatter_sends)
        each(rs_part, 0, (0, 1, 2))
        each(rs_begin, 0, (0,))
        each(rs_part, 0, (3,))
        each(rs_begin, 0, (1,))
        upper(1, 0, 2)
        each(rs_begin, 0, (2, 3))
        upper(1, 1, 2)
        each(rs_part, 1, (0,))
        each(rs_step, 0, 1, (0, 1))
        each(rs_part, 1, (1,))
        each(rs_step, 0, 1, (2, 3))
        each(rs_part, 1, (2,))
        each(rs_begin, 1, (0,))
        each(rs_part, 1, (3,))
        each(rs_begin, 1, (1,))
        each(rs_step, 0, 2, (0, 1))
        each(rs_begin, 1, (2,))
        each(rs_step, 0, 2, (2, 3))
        each(rs_begin, 1, (3,))
        each(rs_step, 1, 1, (0, 1))
        each(rs_step, 0, 3, (0, 1))
        each(rs_step, 1, 1, (2, 3))
        each(rs_step, 0, 3, (2, 3))
        each(rs_step, 1, 2, (0, 1))
        run(rs_final, layer, 0)
        if not final:
            run(layer_norm, layer + 1, 0)
            run(ag_start, layer + 1, 0)
        else:
            store(0).start()
        each(rs_step, 1, 2, (2, 3))
        each(rs_step, 1, 3, (0, 1, 2, 3))
        if not final:
            run(ag_hop, layer + 1, 0, 1)
        run(rs_final, layer, 1)
        if not final:
            run(layer_norm, layer + 1, 1)
            run(ag_start, layer + 1, 1)
            run(ag_hop, layer + 1, 1, 1)
            for i in range(4):
                run(weight_wait, layer + 1, i)
    store(1).start()
    run(drain, scatter_sends)
    run(drain, gather_sends)
    for x in range(2):
        store(x).wait()


def solution(mesh):
    tp = mesh.shape["tp"]
    n_chips = tp // 2
    head_spec = P(None, None, "tp", None)
    head_bias_spec = P(None, "tp", None)
    in_specs = (P("dp", "tp", None), P(), P(), head_spec, head_bias_spec, head_spec, head_bias_spec, head_spec, head_bias_spec,
                P(None, "tp", None, None), P(), P(None, None, "tp"), P(None, "tp"), P(None, "tp", None), P())

    def local_program(x_loc, ln_gain, ln_bias, w_q, b_q, w_k, b_k, w_v, b_v, w_o, b_o, w_up, b_up, w_down, b_down):
        n_layers, width, _, head = w_q.shape
        ff = w_up.shape[2]
        rows = x_loc.shape[1] // 2
        m_rows = 2 * n_chips * rows
        positions = row_positions(n_chips, rows)
        rot = jnp.asarray(rotary_constants(positions))
        mask = jnp.asarray((positions[:, None] >= positions[None, :]).astype(np.float32))
        flat = lambda w: w.reshape(n_layers, width, head)
        bias = lambda b: b.reshape(n_layers, head)
        cfg = (n_layers, n_chips, rows, width, head, ff)
        any_spec = pl.BlockSpec(memory_space=pl.ANY)
        vmem_spec = pl.BlockSpec(memory_space=pltpu.VMEM)
        dma = pltpu.SemaphoreType.DMA
        hops = n_chips // 2
        return pl.pallas_call(
            functools.partial(kernel, cfg),
            out_shape=jax.ShapeDtypeStruct(x_loc.shape, x_loc.dtype),
            in_specs=[any_spec, vmem_spec, vmem_spec] + [any_spec] * 6 + [vmem_spec] * 6 + [any_spec] * 2,
            out_specs=any_spec,
            scratch_shapes=[
                pltpu.VMEM((2 * rows, width), BF16),
                pltpu.VMEM((n_layers, 2, 2, n_chips, rows, width), BF16),
                pltpu.VMEM((2, 2, n_chips, rows, width), BF16),
                pltpu.VMEM((n_layers, 2, n_chips, rows, width), BF16),
                pltpu.VMEM((n_layers, 2, 2, hops, rows, width), BF16),
                pltpu.VMEM((n_layers, width, 3 * head + ff), BF16),
                pltpu.VMEM((n_layers, head + ff, width), BF16),
                pltpu.VMEM((3, 2 * m_rows, head), BF16),
                pltpu.VMEM((2, m_rows, head + ff), BF16),
                pltpu.VMEM((3, 2 * m_rows, 128), F32),
                pltpu.VMEM((2 * m_rows, 2 * m_rows), F32),
                pltpu.VMEM((2 * rows, width), BF16),
                dma((n_layers, 6)),
                dma((5,)),
                dma((n_layers, 2, 2, hops, 2)),
                dma((n_layers, 2, 2, hops, 2)),
                dma((n_layers, 2, n_chips)),
                dma((n_layers, 2, n_chips)),
                dma((n_layers, 2, CHUNKS)),
                dma((n_layers, 2, CHUNKS)),
                dma((n_layers, 2, 2, hops, CHUNKS)),
                dma((n_layers, 2, 2, hops, CHUNKS)),
            ],
            compiler_params=pltpu.CompilerParams(collective_id=0, has_side_effects=True, vmem_limit_bytes=67_000_000),
            name="decoder",
        )(x_loc, ln_gain, ln_bias, flat(w_q), flat(w_k), flat(w_v), w_o.reshape(n_layers, head, width), w_up, w_down,
          bias(b_q), bias(b_k), bias(b_v), b_up, b_o, b_down, rot, mask)

    return jax.shard_map(local_program, mesh=mesh, in_specs=in_specs, out_specs=P("dp", "tp", None), check_vma=False)
```
